32 devices in a mesh: rows: 32 (over z, y, x, core).
Axes of the slice: x: 2, y: 2, z: 4, core: 2. Of those that a mesh axis runs over, the one named last changes fastest.
Arguments:
- source: bfloat16 [65536, 128], P('rows'), may hold values from -6 to 6
- target: bfloat16 [65536, 128], P('rows'), may hold values from -6 to 6
- tile_values: bfloat16 [4096, 128, 128], P('rows'), may hold values from -0.25 to 0.25
- tile_rows: int32 [4096], P('rows'), may hold values from 0 to 15
- tile_peers: int32 [4096], P('rows'), may hold values from 0 to 31
- need_list: int32 [32, 32], P('rows'), may hold values from 0 to 15
- tile_count: int32 [32], P('rows'), may hold values from 1 to 128, as said below
Outputs:
- source_embed: bfloat16 [65536, 128], P('rows')
- target_embed: bfloat16 [65536, 128], P('rows')
The draws below stay inside these ranges and needn't reach their ends.
Inputs may be any that keep to these rules, and one draw needn't show every extreme that they name: `tile_count`: some device has 128 live tiles; tiles in slots at or past the count take no part.
All inputs are finite; a program needn't handle non-finite values.
Results may differ from the reference program's by a relative error of at most 0.0053.
Values may be sent and summed in bfloat16 or wider, within the bound.
A program may use at most 128 MiB of HBM per device.

```python
import math
import jax
import jax.numpy as jnp
import numpy as np
from jax import lax

W = 128
BLOCK = 128
RB = 16
TILES_DEV = 128
ITERS = 2
NODES = 65536
DEVICES = 32


def draw_tile_count(key, part):
    ranks = jax.random.permutation(key, DEVICES)
    counts = TILES_DEV * 16 // (16 + ranks)
    return jnp.maximum(counts, 1).astype(jnp.int32)


def plant(values, rng, least, high):
    longest = values.shape.index(max(values.shape))
    spots = []
    for shift in (0, 1):
        where = [jax.random.randint(jax.random.fold_in(rng, axis), (), 0, length) for axis, length in enumerate(values.shape)]
        where[longest] = (where[longest] + shift) % values.shape[longest]
        spots.append(tuple(where))
    return values.at[spots[0]].set(least).at[spots[1]].set(high)


def levels(stream_key, extent, split, smallest, top_value):
    level, own = 1.0, jax.random.fold_in(stream_key, 6)
    for axis_at, shards_of in split:
        draws = jnp.exp(jax.random.uniform(jax.random.fold_in(own, axis_at), (shards_of,), jnp.float32, smallest / len(split), top_value / len(split)))
        level = level * jnp.repeat(draws, extent[axis_at] // shards_of).reshape([-1 if axis == axis_at else 1 for axis in range(len(extent))])
    return level


def cumulative_ranks(amount, skew):
    portions = [(1 << 20) // math.isqrt(grade ** skew) + 1 for grade in range(1, amount + 1)]
    width = 1 + sum(portions) // (1 << 30)
    return np.cumsum(np.array([max(1, weight // width) for weight in portions]))


def ranked(own_key, shape, count, lean):
    grid = cumulative_ranks(count, lean)
    pick = jax.random.randint(jax.random.fold_in(own_key, 1), shape, 0, int(grid[count - 1]))
    grade = jnp.searchsorted(jnp.asarray(grid, jnp.int32), pick, side="right")
    return jax.random.permutation(jax.random.fold_in(own_key, 2), count)[grade].astype(jnp.int32)


def bell_draw(stream_key, shape, deviation, most, cuts=(), kind=jnp.bfloat16):
    values = deviation * jax.random.normal(stream_key, shape, jnp.float32)
    if cuts:
        values = values * levels(stream_key, shape, cuts, -0.22, 0.18)
    return jnp.clip(values, -most, most).astype(kind)


def setup_inputs(seed: int = 0) -> dict:
    arg_keys = jax.random.split(jax.random.key(seed), 8)
    source = bell_draw(arg_keys[0], (NODES, W), 1.0, 6.0, ((0, 32),))
    target = bell_draw(arg_keys[1], (NODES, W), 1.0, 6.0, ((0, 32),))
    tile_values = bell_draw(arg_keys[2], (DEVICES * TILES_DEV, BLOCK, BLOCK), (BLOCK * 4) ** -0.5, 0.25, ((0, 32),))
    tile_rows = plant(jax.random.randint(arg_keys[3], (DEVICES * TILES_DEV,), 0, RB), jax.random.fold_in(arg_keys[3], 1), 0, RB - 1).astype(jnp.int32)
    tile_peers = plant(ranked(arg_keys[4], (DEVICES * TILES_DEV,), DEVICES, 2), jax.random.fold_in(arg_keys[4], 3), 0, DEVICES - 1).astype(jnp.int32)
    need_list = plant(jax.random.randint(arg_keys[5], (DEVICES, DEVICES), 0, RB), jax.random.fold_in(arg_keys[5], 1), 0, RB - 1).astype(jnp.int32)
    tile_count = draw_tile_count(jax.random.fold_in(arg_keys[7], 71), 0)
    return {"source": source, "target": target, "tile_values": tile_values, "tile_rows": tile_rows, "tile_peers": tile_peers, "need_list": need_list, "tile_count": tile_count}


epsilon = 1e-06

def settle(base, update):
    total = base.astype(jnp.float32) + update
    scale = lax.rsqrt(lax.optimization_barrier(jnp.mean(total * total, axis=-1, keepdims=True)) + epsilon)
    return (total * scale).astype(jnp.bfloat16)

def reference(source, target, tile_values, tile_rows, tile_peers, need_list, tile_count):
    tile_side = tile_values.shape[1]
    feature_width = source.shape[1]
    tiles = tile_values.reshape(DEVICES, TILES_DEV, tile_side, tile_side)
    row_ids = tile_rows.reshape(DEVICES, TILES_DEV).astype(jnp.int32)
    peer_ids = tile_peers.reshape(DEVICES, TILES_DEV).astype(jnp.int32)
    device_ids = jnp.arange(DEVICES, dtype=jnp.int32)[:, None]
    row_blocks = device_ids * RB + row_ids
    col_blocks = peer_ids * RB + jnp.take_along_axis(need_list.astype(jnp.int32), peer_ids, axis=1)
    live_mask = (jnp.arange(TILES_DEV, dtype=jnp.int32)[None, :] < tile_count[:, None]).astype(jnp.float32)
    source_now, target_now = (source, target)
    for iteration in range(ITERS):
        source_blocks = source_now.reshape(-1, tile_side, feature_width).astype(jnp.float32)
        target_blocks = target_now.reshape(-1, tile_side, feature_width).astype(jnp.float32)

        def one_device(target_sum, device):
            tile_block = tiles[device].astype(jnp.float32)
            alive = live_mask[device][:, None, None]
            forward = jnp.einsum('tij,tjk->tik', tile_block, source_blocks[col_blocks[device]], precision=lax.Precision.HIGHEST) * alive
            gathered = jax.ops.segment_sum(forward, row_ids[device], num_segments=RB)
            backward = jnp.einsum('tji,tjk->tik', tile_block, target_blocks[row_blocks[device]], precision=lax.Precision.HIGHEST) * alive
            target_sum = target_sum.at[col_blocks[device]].add(backward)
            return (target_sum, gathered)
        start_sum = jnp.zeros((DEVICES * RB, tile_side, feature_width), jnp.float32)
        target_sum, gathered = lax.scan(one_device, start_sum, jnp.arange(DEVICES, dtype=jnp.int32))
        source_now = settle(source, gathered.reshape(-1, feature_width))
        target_now = settle(target, target_sum.reshape(-1, feature_width))
    return (source_now, target_now)
```

```python
import functools

import jax
import jax.numpy as jnp
from jax import lax
from jax.experimental import pallas as pl
from jax.experimental.pallas import tpu as pltpu
from jax.sharding import PartitionSpec as P

ITERS = 2
UNROLL = 4
epsilon = 1e-06
MESH = pl.DeviceIdType.MESH


def plan_groups(keys, live, groups, per_slot, slots):
    items = keys.shape[0]
    item = jnp.arange(items, dtype=jnp.int32)
    group = jnp.arange(groups, dtype=jnp.int32)
    slot = jnp.arange(slots, dtype=jnp.int32)
    member = (keys[None, :] == group[:, None]) & live[None, :]
    count = jnp.sum(member.astype(jnp.int32), axis=1)
    used = (count + per_slot - 1) // per_slot
    start = jnp.sum(jnp.where(group[None, :] < group[:, None], used[None, :], 0), axis=1)
    same = (keys[None, :] == keys[:, None]) & live[None, :] & (item[None, :] < item[:, None])
    rank = jnp.sum(same.astype(jnp.int32), axis=1)
    first = jnp.sum(jnp.where(keys[:, None] == group[None, :], start[None, :], 0), axis=1)
    place = jnp.where(live, per_slot * first + rank, -1)
    seat = jnp.arange(slots * per_slot, dtype=jnp.int32)
    hot = place[None, :] == seat[:, None]
    filled = jnp.any(hot, axis=1)
    chosen = jnp.sum(jnp.where(hot, item[None, :], 0), axis=1)
    opens = jnp.any((start[None, :] == slot[:, None]) & (used[None, :] > 0), axis=1)
    keep = 1 - opens.astype(jnp.int32)
    last = jnp.where(used > 0, start + used - 1, slots)
    return hot, filled, chosen, keep, last


def pick(hot, filled, values, otherwise):
    return jnp.where(filled, jnp.sum(jnp.where(hot, values[None, :], 0), axis=1), otherwise)


def slots_for(items, groups):
    pairs = (items + min(items, groups)) // 2
    return -(-pairs // UNROLL) * UNROLL


def kernel(
    n,
    offsets,
    f_slots,
    b_slots,
    meta,
    source,
    target,
    tiles,
    source_out,
    target_out,
    x_out,
    x_ins,
    y_out,
    y_ins,
    x_now,
    y_now,
    y_base,
    f_sums,
    b_sums,
    c_sums,
    send_sem,
    recv_sem,
):
    me = lax.axis_index("rows")
    rows, side, width = source.shape
    o = offsets

    barrier = pltpu.get_barrier_semaphore()

    def greet(k, carry):
        pl.semaphore_signal(
            barrier, inc=1, device_id=(lax.rem(me + k, n),), device_id_type=MESH
        )
        return carry

    lax.fori_loop(1, n, greet, 0)

    zero_block = jnp.zeros((side, width), jnp.bfloat16)
    zero_sum = jnp.zeros((side, width), jnp.float32)
    for it in range(ITERS):
        x_ins[it][n] = zero_block
    y_now[rows] = zero_block
    f_sums[f_slots] = zero_sum
    b_sums[b_slots] = zero_block
    c_sums[n] = zero_sum

    def turn(b, carry):
        flipped = target[b].astype(jnp.float32).T
        y_base[b] = flipped
        y_now[b] = flipped.astype(jnp.bfloat16)
        return carry

    lax.fori_loop(0, rows, turn, 0)

    def send(out, inn, phase, it):
        def one(k, carry):
            peer = lax.rem(me + k, n)
            pltpu.make_async_remote_copy(
                src_ref=out.at[it, peer],
                dst_ref=inn.at[me],
                send_sem=send_sem.at[phase],
                recv_sem=recv_sem.at[phase],
                device_id=(peer,),
                device_id_type=MESH,
            ).start()
            return carry

        lax.fori_loop(1, n, one, 0)
        inn[me] = out[it, me]

    def all_of(buffer, sem):
        view = buffer.at[pl.ds(0, n - 1)]
        pltpu.make_async_copy(view, view, sem).wait()

    def send_x(blocks, it):
        def one(p, carry):
            x_out[it, p] = blocks[meta[o["send"] + p]]
            return carry

        lax.fori_loop(0, n, one, 0)
        send(x_out, x_ins[it], 2 * it, it)

    def backward(it):
        def one(q, total):
            left, right = 2 * q, 2 * q + 1
            flipped = jnp.concatenate(
                [y_now[meta[o["b_row"] + left]], y_now[meta[o["b_row"] + right]]], axis=1
            )
            stack = jnp.concatenate(
                [tiles[meta[o["b_tile"] + left]], tiles[meta[o["b_tile"] + right]]], axis=0
            )
            product = jnp.dot(flipped, stack, preferred_element_type=jnp.float32)
            total = total * meta[o["b_keep"] + q].astype(jnp.float32) + product
            b_sums[q] = total.astype(jnp.bfloat16)
            return total

        lax.fori_loop(0, b_slots, one, zero_sum, unroll=UNROLL)

        def place(p, carry):
            y_out[it, p] = b_sums[meta[o["b_last"] + p]]
            return carry

        lax.fori_loop(0, n, place, 0)
        send(y_out, y_ins[it], 2 * it + 1, it)

    def forward(it, result):
        x_in = x_ins[it]
        all_of(x_in, recv_sem.at[2 * it])

        def one(q, total):
            left, right = 2 * q, 2 * q + 1
            stack = jnp.concatenate(
                [tiles[meta[o["f_tile"] + left]], tiles[meta[o["f_tile"] + right]]], axis=1
            )
            blocks = jnp.concatenate(
                [x_in[meta[o["f_peer"] + left]], x_in[meta[o["f_peer"] + right]]], axis=0
            )
            product = jnp.dot(stack, blocks, preferred_element_type=jnp.float32)
            total = total * meta[o["f_keep"] + q].astype(jnp.float32) + product
            f_sums[q] = total
            return total

        lax.fori_loop(0, f_slots, one, zero_sum, unroll=UNROLL)

        def settle(b, carry):
            total = source[b].astype(jnp.float32) + f_sums[meta[o["f_last"] + b]]
            scale = lax.rsqrt(jnp.mean(total * total, axis=-1, keepdims=True) + epsilon)
            result[b] = (total * scale).astype(jnp.bfloat16)
            return carry

        lax.fori_loop(0, rows, settle, 0)

    def combine(it, final):
        y_in = y_ins[it]
        all_of(y_in, recv_sem.at[2 * it + 1])

        def one(k, total):
            part = y_in[meta[o["c_from"] + k]].astype(jnp.float32)
            total = total * meta[o["c_keep"] + k].astype(jnp.float32) + part
            c_sums[k] = total
            return total

        lax.fori_loop(0, n, one, zero_sum)

        def settle(b, carry):
            total = y_base[b] + c_sums[meta[o["c_last"] + b]]
            scale = lax.rsqrt(jnp.mean(total * total, axis=0, keepdims=True) + epsilon)
            if final:
                target_out[b] = (total * scale).T.astype(jnp.bfloat16)
            else:
                y_now[b] = (total * scale).astype(jnp.bfloat16)
            return carry

        lax.fori_loop(0, rows, settle, 0)

    pl.semaphore_wait(barrier, n - 1)
    send_x(source, 0)
    backward(0)
    for it in range(ITERS):
        final = it == ITERS - 1
        forward(it, source_out if final else x_now)
        if not final:
            send_x(x_now, it + 1)
        combine(it, final)
        if not final:
            backward(it + 1)
    for it in range(ITERS):
        all_of(x_out.at[it], send_sem.at[2 * it])
        all_of(y_out.at[it], send_sem.at[2 * it + 1])


def shards(source, target, tile_values, tile_rows, tile_peers, need_list, tile_count):
    n = lax.axis_size("rows")
    tiles_here, side, _ = tile_values.shape
    width = source.shape[1]
    rows = source.shape[0] // side
    live = jnp.arange(tiles_here, dtype=jnp.int32) < tile_count[0]
    send_list = lax.all_to_all(
        need_list.reshape(n, 1), "rows", split_axis=0, concat_axis=0, tiled=True
    )[:, 0]
    f_slots = slots_for(tiles_here, rows)
    b_slots = slots_for(tiles_here, n)
    f_hot, f_filled, f_tile, f_keep, f_last = plan_groups(tile_rows, live, rows, 2, f_slots)
    b_hot, b_filled, b_tile, b_keep, b_last = plan_groups(tile_peers, live, n, 2, b_slots)
    everyone = jnp.ones((n,), jnp.bool_)
    _, _, c_from, c_keep, c_last = plan_groups(send_list, everyone, rows, 1, n)
    pieces = dict(
        f_tile=f_tile,
        f_peer=pick(f_hot, f_filled, tile_peers, n),
        f_keep=f_keep,
        f_last=f_last,
        b_tile=b_tile,
        b_row=pick(b_hot, b_filled, tile_rows, rows),
        b_keep=b_keep,
        b_last=b_last,
        send=send_list,
        c_from=c_from,
        c_keep=c_keep,
        c_last=c_last,
    )
    offsets, at = {}, 0
    for name, piece in pieces.items():
        offsets[name] = at
        at += piece.shape[0]
    meta = jnp.concatenate(list(pieces.values()))
    block = (side, width)
    vmem = pl.BlockSpec(memory_space=pltpu.VMEM)
    source_now, target_now = pl.pallas_call(
        functools.partial(kernel, n, offsets, f_slots, b_slots),
        out_shape=[jax.ShapeDtypeStruct((rows,) + block, jnp.bfloat16)] * 2,
        in_specs=[pl.BlockSpec(memory_space=pltpu.SMEM), vmem, vmem, vmem],
        out_specs=[vmem, vmem],
        scratch_shapes=[
            pltpu.VMEM((ITERS, n) + block, jnp.bfloat16),
            [pltpu.VMEM((n + 1,) + block, jnp.bfloat16)] * ITERS,
            pltpu.VMEM((ITERS, n) + block, jnp.bfloat16),
            [pltpu.VMEM((n,) + block, jnp.bfloat16)] * ITERS,
            pltpu.VMEM((rows,) + block, jnp.bfloat16),
            pltpu.VMEM((rows + 1,) + block, jnp.bfloat16),
            pltpu.VMEM((rows,) + block, jnp.float32),
            pltpu.VMEM((f_slots + 1,) + block, jnp.float32),
            pltpu.VMEM((b_slots + 1,) + block, jnp.bfloat16),
            pltpu.VMEM((n + 1,) + block, jnp.float32),
            pltpu.SemaphoreType.DMA((2 * ITERS,)),
            pltpu.SemaphoreType.DMA((2 * ITERS,)),
        ],
        compiler_params=pltpu.CompilerParams(
            collective_id=0, has_side_effects=True, vmem_limit_bytes=67043328
        ),
    )(
        meta,
        source.reshape((rows,) + block),
        target.reshape((rows,) + block),
        tile_values,
    )
    return source_now.reshape(-1, width), target_now.reshape(-1, width)


def solution(mesh):
    return jax.shard_map(
        shards,
        mesh=mesh,
        in_specs=(
            P("rows", None),
            P("rows", None),
            P("rows", None, None),
            P("rows"),
            P("rows"),
            P("rows", None),
            P("rows"),
        ),
        out_specs=(P("rows", None), P("rows", None)),
        check_vma=False,
    )
```

```python
import functools

import jax
import jax.numpy as jnp
from jax import lax
from jax.experimental import pallas as pl
from jax.experimental.pallas import tpu as pltpu
from jax.sharding import PartitionSpec as P

ITERS = 2
UNROLL = 4
epsilon = 1e-06
MESH = pl.DeviceIdType.MESH


def lanes_for(count):
    return -(-count // 128) * 128


def index_along(shape, axis):
    return lax.broadcasted_iota(jnp.int32, shape, axis).astype(jnp.float32)


def place_groups(keys, groups, per_slot, slots, out, seat_row, last_row):
    items, lanes = keys.shape[1], lanes_for(groups)
    key = jnp.broadcast_to(keys, (items, items))
    key_down = jnp.broadcast_to(keys, (lanes_for(items), items)).T
    before = (key_down[:, :items] == key) & (
        index_along((items, items), 1) < index_along((items, items), 0)
    )
    rank = jnp.sum(before.astype(jnp.float32), axis=1, keepdims=True)
    lane = index_along((items, lanes), 1)
    member = (jnp.broadcast_to(key_down[:, :1], (items, lanes)) == lane).astype(jnp.float32)
    count = jnp.sum(member, axis=0, keepdims=True)
    used = jnp.floor((count + (per_slot - 1)) * (1.0 / per_slot))
    used_down = jnp.broadcast_to(used, (lanes, lanes)).T
    earlier = (index_along((lanes, lanes), 0) < index_along((lanes, lanes), 1)).astype(jnp.float32)
    start = jnp.sum(used_down * earlier, axis=0, keepdims=True)
    last = jnp.where(used > 0, start + used - 1, float(slots))
    first = jnp.sum(member * start, axis=1, keepdims=True)
    place = jnp.where(key_down[:, :1] >= 0, per_slot * first + rank, -1.0)
    seats = lanes_for(slots * per_slot)
    for chunk in range(seats // 128):
        hot = jnp.broadcast_to(place, (items, 128)) == index_along((items, 128), 1) + 128 * chunk
        item = jnp.where(hot, index_along((items, 128), 0) - items, 0.0)
        chosen = items + jnp.sum(item, axis=0, keepdims=True)
        out[pl.ds(seat_row + chunk, 1), :] = chosen.astype(jnp.int32)
    for chunk in range(lanes // 128):
        out[pl.ds(last_row + chunk, 1), :] = last[:, 128 * chunk : 128 * (chunk + 1)].astype(
            jnp.int32
        )


def slots_for(items, groups):
    pairs = (items + min(items, groups)) // 2
    return -(-pairs // UNROLL) * UNROLL


def kernel(
    n,
    f_slots,
    b_slots,
    row_of,
    peer_of,
    live_count,
    rows_lane,
    peers_lane,
    need,
    source,
    target_hbm,
    tiles_hbm,
    source_out,
    target_out,
    x_out,
    x_ins,
    y_out,
    y_ins,
    x_now,
    y_now,
    y_base,
    f_sums,
    b_sums,
    c_sums,
    target,
    tiles,
    need_all,
    need_at,
    tile_plan,
    tile_at,
    part_plan,
    part_at,
    send_sem,
    recv_sem,
    need_send,
    need_recv,
    load_sem,
):
    me = lax.axis_index("rows")
    rows, side, width = source.shape
    tile_total = tiles_hbm.shape[0]
    f_seat, f_last = 0, lanes_for(2 * f_slots) // 128
    b_seat = f_last + lanes_for(rows) // 128
    b_last = b_seat + lanes_for(2 * b_slots) // 128
    c_last = lanes_for(n) // 128

    barrier = pltpu.get_barrier_semaphore()

    def greet(k, carry):
        pl.semaphore_signal(
            barrier, inc=1, device_id=(lax.rem(me + k, n),), device_id_type=MESH
        )
        return carry

    lax.fori_loop(1, n, greet, 0)
    target_load = pltpu.make_async_copy(target_hbm, target, load_sem.at[0])
    target_load.start()
    tile_load = pltpu.make_async_copy(tiles_hbm, tiles.at[pl.ds(0, tile_total)], load_sem.at[1])
    tile_load.start()

    zero_block = jnp.zeros((side, width), jnp.bfloat16)
    zero_sum = jnp.zeros((side, width), jnp.float32)
    tiles[tile_total] = jnp.zeros((side, side), jnp.bfloat16)
    f_sums[f_slots] = zero_sum
    b_sums[b_slots] = zero_block
    c_sums[n] = zero_sum
    need_all[me] = need[...]
    pl.semaphore_wait(barrier, n - 1)

    def ask(k, carry):
        pltpu.make_async_remote_copy(
            src_ref=need,
            dst_ref=need_all.at[me],
            send_sem=need_send.at[0],
            recv_sem=need_recv.at[0],
            device_id=(lax.rem(me + k, n),),
            device_id_type=MESH,
        ).start()
        return carry

    lax.fori_loop(1, n, ask, 0)

    def turn(b, carry):
        flipped = target[b].astype(jnp.float32).T
        y_base[b] = flipped
        y_now[b] = flipped.astype(jnp.bfloat16)
        return carry

    def plan_tiles():
        live = lax.broadcasted_iota(jnp.int32, (1, tile_total), 1) < live_count[0]
        row_keys = jnp.where(live, rows_lane[...], -1).astype(jnp.float32)
        peer_keys = jnp.where(live, peers_lane[...], -1).astype(jnp.float32)
        place_groups(row_keys, rows, 2, f_slots, tile_plan, f_seat, f_last)
        place_groups(peer_keys, n, 2, b_slots, tile_plan, b_seat, b_last)
        load = pltpu.make_async_copy(tile_plan, tile_at, load_sem.at[3])
        load.start()
        load.wait()

    def plan_parts():
        table = need_all[...].reshape(n, need_all.shape[2]).astype(jnp.float32)
        mine = index_along(table.shape, 1) == me.astype(jnp.float32)
        wanted = jnp.sum(jnp.where(mine, table, 0.0), axis=1, keepdims=True)
        keys = jnp.broadcast_to(wanted, (n, 128)).T[:1]
        place_groups(keys, rows, 1, n, part_plan, 0, c_last)
        load = pltpu.make_async_copy(part_plan, part_at, load_sem.at[4])
        load.start()
        load.wait()

    def seat(table, first, index, top):
        return jnp.clip(table[first + index // 128, index % 128], 0, top)

    def tile_pair(first, q):
        left = seat(tile_at, first, 2 * q, tile_total)
        right = seat(tile_at, first, 2 * q + 1, tile_total)
        return left, right, jnp.minimum(left, tile_total - 1), jnp.minimum(right, tile_total - 1)

    def asked(d):
        return jnp.clip(need_at[d, 0, me], 0, rows - 1)

    def send(out, inn, phase, it, fill):
        def one(k, carry):
            peer = lax.rem(me + k, n)
            out[it, peer] = fill(peer)
            pltpu.make_async_remote_copy(
                src_ref=out.at[it, peer],
                dst_ref=inn.at[me],
                send_sem=send_sem.at[phase],
                recv_sem=recv_sem.at[phase],
                device_id=(peer,),
                device_id_type=MESH,
            ).start()
            return carry

        lax.fori_loop(1, n, one, 0)
        inn[me] = fill(me)

    def all_of(buffer, sem):
        view = buffer.at[pl.ds(0, n - 1)]
        pltpu.make_async_copy(view, view, sem).wait()

    def send_x(blocks, it):
        send(x_out, x_ins[it], 2 * it, it, lambda p: blocks[asked(p)])

    def backward(it):
        def one(q, carry):
            total, key = carry
            left, right, left_at, right_at = tile_pair(b_seat, q)
            flipped = jnp.concatenate([y_now[row_of[left_at]], y_now[row_of[right_at]]], axis=1)
            stack = jnp.concatenate([tiles[left], tiles[right]], axis=0)
            product = jnp.dot(flipped, stack, preferred_element_type=jnp.float32)
            new_key = peer_of[left_at]
            total = total * (new_key == key).astype(jnp.float32) + product
            b_sums[q] = total.astype(jnp.bfloat16)
            return total, new_key

        lax.fori_loop(0, b_slots, one, (zero_sum, jnp.int32(-1)), unroll=UNROLL)
        send(y_out, y_ins[it], 2 * it + 1, it, lambda p: b_sums[seat(tile_at, b_last, p, b_slots)])

    def forward(it, result):
        x_in = x_ins[it]
        all_of(x_in, recv_sem.at[2 * it])

        def one(q, carry):
            total, key = carry
            left, right, left_at, right_at = tile_pair(f_seat, q)
            stack = jnp.concatenate([tiles[left], tiles[right]], axis=1)
            blocks = jnp.concatenate([x_in[peer_of[left_at]], x_in[peer_of[right_at]]], axis=0)
            product = jnp.dot(stack, blocks, preferred_element_type=jnp.float32)
            new_key = row_of[left_at]
            total = total * (new_key == key).astype(jnp.float32) + product
            f_sums[q] = total
            return total, new_key

        lax.fori_loop(0, f_slots, one, (zero_sum, jnp.int32(-1)), unroll=UNROLL)

        def settle(b, carry):
            total = source[b].astype(jnp.float32) + f_sums[seat(tile_at, f_last, b, f_slots)]
            scale = lax.rsqrt(jnp.mean(total * total, axis=-1, keepdims=True) + epsilon)
            result[b] = (total * scale).astype(jnp.bfloat16)
            return carry

        lax.fori_loop(0, rows, settle, 0)

    def combine(it, final):
        y_in = y_ins[it]
        all_of(y_in, recv_sem.at[2 * it + 1])

        def one(k, carry):
            total, key = carry
            sender = seat(part_at, 0, k, n - 1)
            new_key = asked(sender)
            total = total * (new_key == key).astype(jnp.float32) + y_in[sender].astype(jnp.float32)
            c_sums[k] = total
            return total, new_key

        lax.fori_loop(0, n, one, (zero_sum, jnp.int32(-1)), unroll=UNROLL)

        def settle(b, carry):
            total = y_base[b] + c_sums[seat(part_at, c_last, b, n)]
            scale = lax.rsqrt(jnp.mean(total * total, axis=0, keepdims=True) + epsilon)
            if final:
                target_out[b] = (total * scale).T.astype(jnp.bfloat16)
            else:
                y_now[b] = (total * scale).astype(jnp.bfloat16)
            return carry

        lax.fori_loop(0, rows, settle, 0)

    all_of(need_all, need_recv.at[0])
    need_load = pltpu.make_async_copy(need_all, need_at, load_sem.at[2])
    need_load.start()
    need_load.wait()
    send_x(source, 0)
    plan_tiles()
    target_load.wait()
    lax.fori_loop(0, rows, turn, 0)
    tile_load.wait()
    backward(0)
    plan_parts()
    for it in range(ITERS):
        final = it == ITERS - 1
        forward(it, source_out if final else x_now)
        if not final:
            send_x(x_now, it + 1)
        combine(it, final)
        if not final:
            backward(it + 1)
    all_of(need_all, need_send.at[0])
    for it in range(ITERS):
        all_of(x_out.at[it], send_sem.at[2 * it])
        all_of(y_out.at[it], send_sem.at[2 * it + 1])


def shards(source, target, tile_values, tile_rows, tile_peers, need_list, tile_count):
    n = lax.axis_size("rows")
    tiles_here, side, _ = tile_values.shape
    width = source.shape[1]
    rows = source.shape[0] // side
    f_slots = slots_for(tiles_here, rows)
    b_slots = slots_for(tiles_here, n)
    tile_plan = (
        lanes_for(2 * f_slots) + lanes_for(rows) + lanes_for(2 * b_slots) + lanes_for(n)
    ) // 128
    part_plan = (lanes_for(n) + lanes_for(rows)) // 128
    wide = lanes_for(n)
    need = jnp.pad(need_list.reshape(1, n), ((0, 0), (0, wide - n)))
    block = (side, width)
    vmem = pl.BlockSpec(memory_space=pltpu.VMEM)
    smem = pl.BlockSpec(memory_space=pltpu.SMEM)
    source_now, target_now = pl.pallas_call(
        functools.partial(kernel, n, f_slots, b_slots),
        out_shape=[jax.ShapeDtypeStruct((rows,) + block, jnp.bfloat16)] * 2,
        in_specs=[smem] * 3 + [vmem] * 4 + [pl.BlockSpec(memory_space=pl.ANY)] * 2,
        out_specs=[vmem, vmem],
        scratch_shapes=[
            pltpu.VMEM((ITERS, n) + block, jnp.bfloat16),
            [pltpu.VMEM((n,) + block, jnp.bfloat16)] * ITERS,
            pltpu.VMEM((ITERS, n) + block, jnp.bfloat16),
            [pltpu.VMEM((n,) + block, jnp.bfloat16)] * ITERS,
            pltpu.VMEM((rows,) + block, jnp.bfloat16),
            pltpu.VMEM((rows,) + block, jnp.bfloat16),
            pltpu.VMEM((rows,) + block, jnp.float32),
            pltpu.VMEM((f_slots + 1,) + block, jnp.float32),
            pltpu.VMEM((b_slots + 1,) + block, jnp.bfloat16),
            pltpu.VMEM((n + 1,) + block, jnp.float32),
            pltpu.VMEM((rows,) + block, jnp.bfloat16),
            pltpu.VMEM((tiles_here + 1, side, side), jnp.bfloat16),
            pltpu.VMEM((n, 1, wide), jnp.int32),
            pltpu.SMEM((n, 1, wide), jnp.int32),
            pltpu.VMEM((tile_plan, 128), jnp.int32),
            pltpu.SMEM((tile_plan, 128), jnp.int32),
            pltpu.VMEM((part_plan, 128), jnp.int32),
            pltpu.SMEM((part_plan, 128), jnp.int32),
            pltpu.SemaphoreType.DMA((2 * ITERS,)),
            pltpu.SemaphoreType.DMA((2 * ITERS,)),
            pltpu.SemaphoreType.DMA((1,)),
            pltpu.SemaphoreType.DMA((1,)),
            pltpu.SemaphoreType.DMA((5,)),
        ],
        compiler_params=pltpu.CompilerParams(
            collective_id=0, has_side_effects=True, vmem_limit_bytes=67043328
        ),
    )(
        tile_rows,
        tile_peers,
        tile_count,
        tile_rows.reshape(1, -1),
        tile_peers.reshape(1, -1),
        need,
        source.reshape((rows,) + block),
        target.reshape((rows,) + block),
        tile_values,
    )
    return source_now.reshape(-1, width), target_now.reshape(-1, width)


def solution(mesh):
    return jax.shard_map(
        shards,
        mesh=mesh,
        in_specs=(
            P("rows", None),
            P("rows", None),
            P("rows", None, None),
            P("rows"),
            P("rows"),
            P("rows", None),
            P("rows"),
        ),
        out_specs=(P("rows", None), P("rows", None)),
        check_vma=False,
    )
```

```python
import functools

import jax
import jax.numpy as jnp
from jax import lax
from jax.experimental import pallas as pl
from jax.experimental.pallas import tpu as pltpu
from jax.sharding import PartitionSpec as P

ITERS = 2
UNROLL = 4
epsilon = 1e-06
MESH = pl.DeviceIdType.MESH


def lanes_for(count):
    return -(-count // 128) * 128


def index_along(shape, axis):
    return lax.broadcasted_iota(jnp.int32, shape, axis).astype(jnp.float32)


def place_groups(keys, groups, per_slot, slots, out, seat_row, last_row):
    items, lanes = keys.shape[1], lanes_for(groups)
    key = jnp.broadcast_to(keys, (items, items))
    key_down = jnp.broadcast_to(keys, (lanes_for(items), items)).T
    before = (key_down[:, :items] == key) & (
        index_along((items, items), 1) < index_along((items, items), 0)
    )
    rank = jnp.sum(before.astype(jnp.float32), axis=1, keepdims=True)
    lane = index_along((items, lanes), 1)
    member = (jnp.broadcast_to(key_down[:, :1], (items, lanes)) == lane).astype(jnp.float32)
    count = jnp.sum(member, axis=0, keepdims=True)
    used = jnp.floor((count + (per_slot - 1)) * (1.0 / per_slot))
    used_down = jnp.broadcast_to(used, (lanes, lanes)).T
    earlier = (index_along((lanes, lanes), 0) < index_along((lanes, lanes), 1)).astype(jnp.float32)
    start = jnp.sum(used_down * earlier, axis=0, keepdims=True)
    last = jnp.where(used > 0, start + used - 1, float(slots))
    first = jnp.sum(member * start, axis=1, keepdims=True)
    place = jnp.where(key_down[:, :1] >= 0, per_slot * first + rank, -1.0)
    seats = lanes_for(slots * per_slot)
    for chunk in range(seats // 128):
        hot = jnp.broadcast_to(place, (items, 128)) == index_along((items, 128), 1) + 128 * chunk
        item = jnp.where(hot, index_along((items, 128), 0) - items, 0.0)
        chosen = items + jnp.sum(item, axis=0, keepdims=True)
        out[pl.ds(seat_row + chunk, 1), :] = chosen.astype(jnp.int32)
    for chunk in range(lanes // 128):
        out[pl.ds(last_row + chunk, 1), :] = last[:, 128 * chunk : 128 * (chunk + 1)].astype(
            jnp.int32
        )


def slots_for(items, groups):
    pairs = (items + min(items, groups)) // 2
    return -(-pairs // UNROLL) * UNROLL


def kernel(
    n,
    f_slots,
    b_slots,
    row_of,
    peer_of,
    live_count,
    rows_lane,
    peers_lane,
    need,
    source_hbm,
    target_hbm,
    tiles_hbm,
    source_out,
    target_out,
    x_out,
    x_ins,
    y_out,
    y_ins,
    x_now,
    y_now,
    y_base,
    f_sums,
    b_sums,
    c_sums,
    source,
    target,
    tiles,
    need_all,
    need_at,
    tile_plan,
    tile_at,
    part_plan,
    part_at,
    send_sem,
    recv_sem,
    need_send,
    need_recv,
    load_sem,
):
    me = lax.axis_index("rows")
    rows, side, width = source.shape
    tile_total = tiles_hbm.shape[0]
    f_seat, f_last = 0, lanes_for(2 * f_slots) // 128
    b_seat = f_last + lanes_for(rows) // 128
    b_last = b_seat + lanes_for(2 * b_slots) // 128
    c_last = lanes_for(n) // 128

    barrier = pltpu.get_barrier_semaphore()

    def greet(k, carry):
        pl.semaphore_signal(
            barrier, inc=1, device_id=(lax.rem(me + k, n),), device_id_type=MESH
        )
        return carry

    lax.fori_loop(1, n, greet, 0)
    source_load = pltpu.make_async_copy(source_hbm, source, load_sem.at[5])
    source_load.start()
    target_load = pltpu.make_async_copy(target_hbm, target, load_sem.at[0])
    target_load.start()
    tile_load = pltpu.make_async_copy(tiles_hbm, tiles.at[pl.ds(0, tile_total)], load_sem.at[1])
    tile_load.start()

    zero_block = jnp.zeros((side, width), jnp.bfloat16)
    zero_sum = jnp.zeros((side, width), jnp.float32)
    tiles[tile_total] = jnp.zeros((side, side), jnp.bfloat16)
    f_sums[f_slots] = zero_sum
    b_sums[b_slots] = zero_block
    c_sums[n] = zero_sum
    need_all[me] = need[...]
    pl.semaphore_wait(barrier, n - 1)

    def ask(k, carry):
        pltpu.make_async_remote_copy(
            src_ref=need,
            dst_ref=need_all.at[me],
            send_sem=need_send.at[0],
            recv_sem=need_recv.at[0],
            device_id=(lax.rem(me + k, n),),
            device_id_type=MESH,
        ).start()
        return carry

    lax.fori_loop(1, n, ask, 0)

    def turn(b, carry):
        flipped = target[b].astype(jnp.float32).T
        y_base[b] = flipped
        y_now[b] = flipped.astype(jnp.bfloat16)
        return carry

    def plan_tiles():
        live = lax.broadcasted_iota(jnp.int32, (1, tile_total), 1) < live_count[0]
        row_keys = jnp.where(live, rows_lane[...], -1).astype(jnp.float32)
        peer_keys = jnp.where(live, peers_lane[...], -1).astype(jnp.float32)
        place_groups(row_keys, rows, 2, f_slots, tile_plan, f_seat, f_last)
        place_groups(peer_keys, n, 2, b_slots, tile_plan, b_seat, b_last)
        load = pltpu.make_async_copy(tile_plan, tile_at, load_sem.at[3])
        load.start()
        load.wait()

    def plan_parts():
        table = need_all[...].reshape(n, need_all.shape[2]).astype(jnp.float32)
        mine = index_along(table.shape, 1) == me.astype(jnp.float32)
        wanted = jnp.sum(jnp.where(mine, table, 0.0), axis=1, keepdims=True)
        keys = jnp.broadcast_to(wanted, (n, 128)).T[:1]
        place_groups(keys, rows, 1, n, part_plan, 0, c_last)
        load = pltpu.make_async_copy(part_plan, part_at, load_sem.at[4])
        load.start()
        load.wait()

    def seat(table, first, index, top):
        return jnp.clip(table[first + index // 128, index % 128], 0, top)

    def tile_pair(first, q):
        left = seat(tile_at, first, 2 * q, tile_total)
        right = seat(tile_at, first, 2 * q + 1, tile_total)
        return left, right, jnp.minimum(left, tile_total - 1), jnp.minimum(right, tile_total - 1)

    def asked(d):
        return jnp.clip(need_at[d, 0, me], 0, rows - 1)

    def send(out, inn, phase, it, fill):
        def one(k, carry):
            peer = lax.rem(me + k, n)
            out[it, peer] = fill(peer)
            pltpu.make_async_remote_copy(
                src_ref=out.at[it, peer],
                dst_ref=inn.at[me],
                send_sem=send_sem.at[phase],
                recv_sem=recv_sem.at[phase],
                device_id=(peer,),
                device_id_type=MESH,
            ).start()
            return carry

        lax.fori_loop(1, n, one, 0)
        inn[me] = fill(me)

    def all_of(buffer, sem):
        view = buffer.at[pl.ds(0, n - 1)]
        pltpu.make_async_copy(view, view, sem).wait()

    def send_x(blocks, it):
        send(x_out, x_ins[it], 2 * it, it, lambda p: blocks[asked(p)])

    def backward(it):
        def one(q, carry):
            total, key = carry
            left, right, left_at, right_at = tile_pair(b_seat, q)
            flipped = jnp.concatenate([y_now[row_of[left_at]], y_now[row_of[right_at]]], axis=1)
            stack = jnp.concatenate([tiles[left], tiles[right]], axis=0)
            product = jnp.dot(flipped, stack, preferred_element_type=jnp.float32)
            new_key = peer_of[left_at]
            total = total * (new_key == key).astype(jnp.float32) + product
            b_sums[q] = total.astype(jnp.bfloat16)
            return total, new_key

        lax.fori_loop(0, b_slots, one, (zero_sum, jnp.int32(-1)), unroll=UNROLL)
        send(y_out, y_ins[it], 2 * it + 1, it, lambda p: b_sums[seat(tile_at, b_last, p, b_slots)])

    def forward(it, result):
        x_in = x_ins[it]
        all_of(x_in, recv_sem.at[2 * it])

        def one(q, carry):
            total, key = carry
            left, right, left_at, right_at = tile_pair(f_seat, q)
            stack = jnp.concatenate([tiles[left], tiles[right]], axis=1)
            blocks = jnp.concatenate([x_in[peer_of[left_at]], x_in[peer_of[right_at]]], axis=0)
            product = jnp.dot(stack, blocks, preferred_element_type=jnp.float32)
            new_key = row_of[left_at]
            total = total * (new_key == key).astype(jnp.float32) + product
            f_sums[q] = total
            return total, new_key

        lax.fori_loop(0, f_slots, one, (zero_sum, jnp.int32(-1)), unroll=UNROLL)

        def settle(b, carry):
            total = source[b].astype(jnp.float32) + f_sums[seat(tile_at, f_last, b, f_slots)]
            scale = lax.rsqrt(jnp.mean(total * total, axis=-1, keepdims=True) + epsilon)
            result[b] = (total * scale).astype(jnp.bfloat16)
            return carry

        lax.fori_loop(0, rows, settle, 0)

    def combine(it, final):
        y_in = y_ins[it]
        all_of(y_in, recv_sem.at[2 * it + 1])

        def one(k, carry):
            total, key = carry
            sender = seat(part_at, 0, k, n - 1)
            new_key = asked(sender)
            total = total * (new_key == key).astype(jnp.float32) + y_in[sender].astype(jnp.float32)
            c_sums[k] = total
            return total, new_key

        lax.fori_loop(0, n, one, (zero_sum, jnp.int32(-1)), unroll=UNROLL)

        def settle(b, carry):
            total = y_base[b] + c_sums[seat(part_at, c_last, b, n)]
            scale = lax.rsqrt(jnp.mean(total * total, axis=0, keepdims=True) + epsilon)
            if final:
                target_out[b] = (total * scale).T.astype(jnp.bfloat16)
            else:
                y_now[b] = (total * scale).astype(jnp.bfloat16)
            return carry

        lax.fori_loop(0, rows, settle, 0)

    all_of(need_all, need_recv.at[0])
    need_load = pltpu.make_async_copy(need_all, need_at, load_sem.at[2])
    need_load.start()
    need_load.wait()
    source_load.wait()
    send_x(source, 0)
    plan_tiles()
    target_load.wait()
    lax.fori_loop(0, rows, turn, 0)
    tile_load.wait()
    backward(0)
    plan_parts()
    for it in range(ITERS):
        final = it == ITERS - 1
        forward(it, source_out if final else x_now)
        if not final:
            send_x(x_now, it + 1)
        combine(it, final)
        if not final:
            backward(it + 1)
    all_of(need_all, need_send.at[0])
    for it in range(ITERS):
        all_of(x_out.at[it], send_sem.at[2 * it])
        all_of(y_out.at[it], send_sem.at[2 * it + 1])


def shards(source, target, tile_values, tile_rows, tile_peers, need_list, tile_count):
    n = lax.axis_size("rows")
    tiles_here, side, _ = tile_values.shape
    width = source.shape[1]
    rows = source.shape[0] // side
    f_slots = slots_for(tiles_here, rows)
    b_slots = slots_for(tiles_here, n)
    tile_plan = (
        lanes_for(2 * f_slots) + lanes_for(rows) + lanes_for(2 * b_slots) + lanes_for(n)
    ) // 128
    part_plan = (lanes_for(n) + lanes_for(rows)) // 128
    block = (side, width)
    vmem = pl.BlockSpec(memory_space=pltpu.VMEM)
    smem = pl.BlockSpec(memory_space=pltpu.SMEM)
    source_now, target_now = pl.pallas_call(
        functools.partial(kernel, n, f_slots, b_slots),
        out_shape=[jax.ShapeDtypeStruct((rows,) + block, jnp.bfloat16)] * 2,
        in_specs=[smem] * 3 + [vmem] * 3 + [pl.BlockSpec(memory_space=pltpu.HBM)] * 3,
        out_specs=[vmem, vmem],
        scratch_shapes=[
            pltpu.VMEM((ITERS, n) + block, jnp.bfloat16),
            [pltpu.VMEM((n,) + block, jnp.bfloat16)] * ITERS,
            pltpu.VMEM((ITERS, n) + block, jnp.bfloat16),
            [pltpu.VMEM((n,) + block, jnp.bfloat16)] * ITERS,
            pltpu.VMEM((rows,) + block, jnp.bfloat16),
            pltpu.VMEM((rows,) + block, jnp.bfloat16),
            pltpu.VMEM((rows,) + block, jnp.float32),
            pltpu.VMEM((f_slots + 1,) + block, jnp.float32),
            pltpu.VMEM((b_slots + 1,) + block, jnp.bfloat16),
            pltpu.VMEM((n + 1,) + block, jnp.float32),
            pltpu.VMEM((rows,) + block, jnp.bfloat16),
            pltpu.VMEM((rows,) + block, jnp.bfloat16),
            pltpu.VMEM((tiles_here + 1, side, side), jnp.bfloat16),
            pltpu.VMEM((n, 1, n), jnp.int32),
            pltpu.SMEM((n, 1, n), jnp.int32),
            pltpu.VMEM((tile_plan, 128), jnp.int32),
            pltpu.SMEM((tile_plan, 128), jnp.int32),
            pltpu.VMEM((part_plan, 128), jnp.int32),
            pltpu.SMEM((part_plan, 128), jnp.int32),
            pltpu.SemaphoreType.DMA((2 * ITERS,)),
            pltpu.SemaphoreType.DMA((2 * ITERS,)),
            pltpu.SemaphoreType.DMA((1,)),
            pltpu.SemaphoreType.DMA((1,)),
            pltpu.SemaphoreType.DMA((6,)),
        ],
        compiler_params=pltpu.CompilerParams(
            collective_id=0, has_side_effects=True, vmem_limit_bytes=67043328
        ),
    )(
        tile_rows,
        tile_peers,
        tile_count,
        tile_rows.reshape(1, -1),
        tile_peers.reshape(1, -1),
        need_list,
        source.reshape((rows,) + block),
        target.reshape((rows,) + block),
        tile_values,
    )
    return source_now.reshape(-1, width), target_now.reshape(-1, width)


def solution(mesh):
    return jax.shard_map(
        shards,
        mesh=mesh,
        in_specs=(
            P("rows", None),
            P("rows", None),
            P("rows", None, None),
            P("rows"),
            P("rows"),
            P("rows", None),
            P("rows"),
        ),
        out_specs=(P("rows", None), P("rows", None)),
        check_vma=False,
    )
```
